32 devices in a mesh: rep: 4 (over x, y), dp: 8 (over z, core).
Axes of the slice: x: 2, y: 2, z: 4, core: 2. Of those that a mesh axis runs over, the one named last changes fastest.
Arguments:
- x: bfloat16 [32, 2048, 896], P(('rep', 'dp')), parts along dimension 0
- dy: bfloat16 [32, 2048, 896], P(('rep', 'dp')), parts along dimension 0
- wq: bfloat16 [2, 896, 896], P(None, 'dp')
- wk: bfloat16 [2, 896, 128], P(None, 'dp')
- wv: bfloat16 [2, 896, 128], P(None, 'dp')
- wo: bfloat16 [2, 896, 896], P(None, 'dp')
- w_gate: bfloat16 [2, 896, 2560], P(None, 'dp')
- w_up: bfloat16 [2, 896, 2560], P(None, 'dp')
- w_down: bfloat16 [2, 2560, 896], P(None, 'dp')
Outputs:
- output 1: bfloat16 [32, 2048, 896], P(('rep', 'dp')), parts along dimension 0
- output 2: bfloat16 [8, 896, 896], P('rep', 'dp'), parts along dimension 0
- output 3: bfloat16 [8, 896, 128], P('rep', 'dp'), parts along dimension 0
- output 4: bfloat16 [8, 896, 128], P('rep', 'dp'), parts along dimension 0
- output 5: bfloat16 [8, 896, 896], P('rep', 'dp'), parts along dimension 0
- output 6: bfloat16 [8, 896, 2560], P('rep', 'dp'), parts along dimension 0
- output 7: bfloat16 [8, 896, 2560], P('rep', 'dp'), parts along dimension 0
- output 8: bfloat16 [8, 2560, 896], P('rep', 'dp'), parts along dimension 0
There are 4 independent parts. The reference program is written for one: setup_inputs(seed, part) draws one part's arguments, and reference() takes and returns one part's arrays. A program takes and returns all parts, laid end to end along the dimension named above; an argument that names none is the same for every part.
All inputs are finite; a program needn't handle non-finite values.
Results may differ from the reference program's by a relative error of at most 0.0278.
Values are sent between devices in bfloat16 or wider.
A program may use at most 2 GiB of HBM per device.

```python
import jax
import jax.numpy as jnp
from jax import lax

SEQUENCES = 8
TOKENS = 2048
D = 896
HEADS = 7
KV_HEADS = 1
HEAD = 128
FF = 2560
LAYERS = 2
THETA = 10000
NAMES = ("wq", "wk", "wv", "wo", "w_gate", "w_up", "w_down")
SHAPES = {
    "wq": (LAYERS, D, HEADS * HEAD),
    "wk": (LAYERS, D, KV_HEADS * HEAD),
    "wv": (LAYERS, D, KV_HEADS * HEAD),
    "wo": (LAYERS, HEADS * HEAD, D),
    "w_gate": (LAYERS, D, FF),
    "w_up": (LAYERS, D, FF),
    "w_down": (LAYERS, FF, D),
}


def bump(key, n, height):
    away = (jnp.arange(n, dtype=jnp.int32) - jax.random.randint(key, (), 0, n, jnp.int32)) % n
    return jnp.where(away < n // 8, height, 1.0)


def together(key, own, strength):
    shared = jax.random.normal(key, own.shape[1:], jnp.float32)
    return (own + strength * shared) * lax.rsqrt(1 + strength * strength)


def setup_inputs(seed: int = 0, part: int = 0) -> dict:
    kx, kdy, ka, kb, kz, kf, kh, kl, *keys = jax.random.split(jax.random.key(seed), 8 + 3 * len(NAMES))
    kx, kdy, ka, kb = (jax.random.fold_in(k, part) for k in (kx, kdy, ka, kb))
    kw, km, kv = (keys[i::3] for i in range(3))
    shape = (SEQUENCES, TOKENS, D)
    much_x, much_dy = jax.random.uniform(kz, (2,), jnp.float32, 0.0, 1.0)
    loud = 2.0 ** jax.random.uniform(jax.random.fold_in(kz, 1), (), jnp.float32, -1.0, 2.0)
    layers = 2.0 ** jax.random.uniform(kl, (LAYERS, 1, 1), jnp.float32, -1.0, 1.0)
    times = {"wq": 1.0, "wk": 1.0, "wv": 2.0, "wo": layers, "w_gate": 1.0, "w_up": bump(kh, FF, 4.0), "w_down": layers}
    x = together(ka, jax.random.normal(kx, shape, jnp.float32), much_x) * bump(kf, D, 4.0)
    dy = together(kb, jax.random.normal(kdy, shape, jnp.float32), much_dy)
    drawn = {"x": x.astype(jnp.bfloat16), "dy": (loud * dy * (SEQUENCES * TOKENS) ** -0.5).astype(jnp.bfloat16)}
    for key, name in zip(kw, NAMES, strict=True):
        drawn[name] = (jax.random.normal(key, SHAPES[name], jnp.float32) * SHAPES[name][1] ** -0.5 * times[name]).astype(jnp.bfloat16)
    return drawn


def matmul(a, w):
    return jnp.dot(a, w, preferred_element_type=jnp.float32).astype(jnp.bfloat16)


def normed(h):
    wide = h.astype(jnp.float32)
    scale = lax.rsqrt(jnp.mean(wide**2, -1, keepdims=True) + 1e-6)
    return (wide * scale).astype(jnp.bfloat16)


def turned(t, theta):
    half = t.shape[-1] // 2
    angle = jnp.arange(t.shape[0], dtype=jnp.float32)[:, None] * theta ** (-jnp.arange(half, dtype=jnp.float32) / half)
    cos, sin = jnp.cos(angle)[:, None], jnp.sin(angle)[:, None]
    a, b = t[..., :half].astype(jnp.float32), t[..., half:].astype(jnp.float32)
    return jnp.concatenate([a * cos - b * sin, b * cos + a * sin], -1).astype(jnp.bfloat16)


def seen_by(q, k, v):
    tokens, kv = q.shape[0], k.shape[1]
    q = q.reshape(tokens, kv, -1, q.shape[-1])
    scores = jnp.einsum("tgsd,ugd->gstu", q.astype(jnp.float32), k.astype(jnp.float32)) * q.shape[-1] ** -0.5
    place = jnp.arange(tokens)
    weights = jax.nn.softmax(jnp.where(place[:, None] >= place, scores, -jnp.inf), -1).astype(jnp.bfloat16)
    return jnp.einsum("gstu,ugd->tgsd", weights.astype(jnp.float32), v.astype(jnp.float32)).astype(jnp.bfloat16).reshape(tokens, -1)


def layer(h, w):
    a = normed(h)
    q, k = (turned(matmul(a, w[name]).reshape(h.shape[0], -1, HEAD), THETA) for name in ("wq", "wk"))
    h = h + matmul(seen_by(q, k, matmul(a, w["wv"]).reshape(h.shape[0], -1, HEAD)), w["wo"])
    b = normed(h)
    gate = jnp.dot(b, w["w_gate"], preferred_element_type=jnp.float32)
    up = jnp.dot(b, w["w_up"], preferred_element_type=jnp.float32)
    return h + matmul((jax.nn.silu(gate) * up).astype(jnp.bfloat16), w["w_down"])


def stack(weights, h):
    return lax.scan(lambda h, w: (layer(h, w), None), h, weights)[0]


def reference(x, dy, wq, wk, wv, wo, w_gate, w_up, w_down):
    weights = dict(zip(NAMES, (wq, wk, wv, wo, w_gate, w_up, w_down), strict=True))

    def take(so_far, sequence):
        h, by_y = sequence
        _, back = jax.vjp(stack, weights, h)
        by_weights, by_h = back(by_y)
        return jax.tree.map(lambda total, term: total + term.astype(jnp.float32), so_far, by_weights), by_h

    none_yet = {name: jnp.zeros(w.shape, jnp.float32) for name, w in weights.items()}
    by_weights, by_x = lax.scan(take, none_yet, (x, dy))
    return (by_x, *(by_weights[name].astype(jnp.bfloat16) for name in NAMES))
```

```python
import functools

import jax
import jax.numpy as jnp
from jax import lax
from jax.experimental import pallas as pl
from jax.experimental.pallas import tpu as pltpu
from jax.sharding import PartitionSpec as P


HEAD = 128
THETA = 10000
LOG2E = 1.4426950408889634
NEG = -1e30
HIDDEN = 2 * NEG
VMEM = 60 * 2**20
MESH = pl.DeviceIdType.MESH
REPS = 4
LOW, WIDE = jnp.bfloat16, jnp.float32


def _dot(a, b, ca=1, cb=0):
    return lax.dot_general(a, b, (((ca,), (cb,)), ((), ())), preferred_element_type=WIDE)


def _scale(x):
    return lax.rsqrt(jnp.mean(x * x, -1, keepdims=True) + 1e-6)


def _norm(h):
    x = h.astype(WIDE)
    return (x * _scale(x)).astype(LOW)


def _norm_bwd(h, d):
    x, d = h.astype(WIDE), d.astype(WIDE)
    s = _scale(x)
    along = jnp.sum(d * x, -1, keepdims=True) * (s * s * s * (1 / x.shape[-1]))
    return (d * s - x * along).astype(LOW)


def _add(a, b):
    return (a.astype(WIDE) + b.astype(WIDE)).astype(LOW)


def _turn(t, cos, sin):
    return (t * cos + pltpu.roll(t, HEAD // 2, 1) * sin).astype(LOW)


class Gather:
    TRANSFERS = 19

    def __init__(self, pieces, outs, kinds, send, recv, local):
        self.pieces, self.outs, self.kinds, self.send, self.recv, self.local = pieces, outs, kinds, send, recv, local
        self.r, dp = lax.axis_index("rep"), lax.axis_index("dp")
        self.z, self.c = dp // 2, dp % 2
        self.rx, self.ry, self.rd = (self.r + 2) % 4, self.r + 1 - 2 * (self.r % 2), 3 - self.r

    def greet(self):
        barrier = pltpu.get_barrier_semaphore()
        here = self.z * 2 + self.c
        others = [(self.r, (self.z + k) % 4 * 2 + self.c) for k in (1, 2, 3)]
        others += [(self.rx, here), (self.ry, here), (self.r, self.z * 2 + 1 - self.c)]
        for rep, dp in others:
            pl.semaphore_signal(barrier, inc=1, device_id=(rep, dp), device_id_type=MESH)
        pl.semaphore_wait(barrier, len(others))

    def place(self, m, z, r):
        ref, z = self.outs[m], pl.ds(0, 4) if z is None else z
        if self.kinds[m] == "rows":
            return ref.at[z, self.c, r]
        width = self.pieces[m].shape[1]
        return ref.at[z, self.c, :, pl.ds(pl.multiple_of(r * width, 128), width)]

    def copy(self, m, t):
        z, r, rx, ry = self.z, self.r, self.rx, self.ry
        behind = lambda j: (z + 4 - j) % 4
        here = z * 2 + self.c
        if t < 3:
            of, to = (z, r), (r, (z + t + 1) % 4 * 2 + self.c)
        elif t < 11:
            j = (t - 3) % 4
            of, to = (behind(j), r), (rx if t < 7 else ry, here)
        elif t < 13:
            of, to = (behind(t - 11), rx), (ry, here)
        elif t < 15:
            of, to = (behind(t - 11), ry), (rx, here)
        else:
            of, to = (None, (r, rx, ry, self.rd)[t - 15]), (r, z * 2 + 1 - self.c)
        dst = self.place(m, *of)
        src = self.pieces[m] if t in (0, 1, 2, 3, 7) else dst
        return pltpu.make_async_remote_copy(src_ref=src, dst_ref=dst, send_sem=self.send.at[m, t], recv_sem=self.recv.at[m, t],
                                            device_id=to, device_id_type=MESH)

    def own(self, m):
        return pltpu.make_async_copy(self.pieces[m], self.place(m, self.z, self.r), self.local.at[m])

    def stage(self, m, s):
        start = lambda *ts: [self.copy(m, t).start() for t in ts]
        got = lambda *ts: [self.copy(m, t).wait_recv() for t in ts]
        if s == 0:
            self.own(m).start()
            start(0, 1, 2)
        elif s == 1:
            start(3, 7)
        elif s < 5:
            got(s - 2)
            start(2 + s, 6 + s)
            if s == 4:
                self.own(m).wait()
                start(15)
        elif s == 5:
            got(3, 4)
            start(11, 12)
        elif s == 6:
            got(9, 10)
            start(13, 14)
            got(5, 6)
            start(16)
            got(7, 8)
            start(17)
        elif s == 7:
            got(11, 12, 13, 14)
            start(18)
        else:
            got(15, 16, 17, 18)
            for t in range(self.TRANSFERS):
                self.copy(m, t).wait_send()


def _call(body, grid, ins, outs, scratch=(), flops=0, gather=None, collective_id=None):
    def spec(shape, block, at):
        whole = tuple(block) == tuple(shape)
        return pl.BlockSpec(block, at, pipeline_mode=pl.Buffered(1)) if whole else pl.BlockSpec(block, at)

    size = lambda s, t: functools.reduce(lambda x, y: x * y, s, 1) * jnp.dtype(t).itemsize
    moved = sum(size(a.shape, a.dtype) for a, _, _ in ins) + sum(size(s, t) for s, t, _, _ in outs)
    in_specs, args = [spec(a.shape, block, at) for a, block, at in ins], [a for a, _, _ in ins]
    out_specs = [pl.BlockSpec(block, at) for _, _, block, at in outs]
    out_shape = [jax.ShapeDtypeStruct(s, t) for s, t, _, _ in outs]
    scratch = list(scratch)
    extra = {} if collective_id is None else dict(collective_id=collective_id, has_side_effects=True)
    if gather is not None:
        cid, pieces = gather
        extra = dict(collective_id=cid, has_side_effects=True)
        for kind, array, n in pieces:
            rows, cols = array.shape[1:]
            if kind == "rows":
                block, shape = (rows // REPS, cols), (4, 2, REPS, rows // REPS, cols)
                at = lambda *i, n=n: (n, lax.axis_index("rep"), 0)
            else:
                block, shape = (rows, cols // REPS), (4, 2, rows, cols)
                at = lambda *i, n=n: (n, 0, lax.axis_index("rep"))
            in_specs.append(pl.BlockSpec((1, *block), at, pipeline_mode=pl.Buffered(1)))
            args.append(array)
            out_specs.append(pl.BlockSpec(memory_space=pl.ANY))
            out_shape.append(jax.ShapeDtypeStruct(shape, array.dtype))
        m = len(pieces)
        scratch += [pltpu.SemaphoreType.DMA((m, Gather.TRANSFERS)), pltpu.SemaphoreType.DMA((m, Gather.TRANSFERS)), pltpu.SemaphoreType.DMA((m,))]
        inner, n_in, n_out = body, len(ins), len(outs)

        def body(*refs):
            mine, refs = refs[:n_in], refs[n_in:]
            parts, refs = refs[:m], refs[m:]
            results, refs = refs[:n_out], refs[n_out:]
            whole, refs = refs[:m], refs[m:]
            inner(Gather([p.at[0] for p in parts], whole, [k for k, _, _ in pieces], *refs[-3:]), *mine, *results, *refs[:-3])

    return pl.pallas_call(
        body,
        grid=grid,
        in_specs=in_specs,
        out_specs=out_specs,
        out_shape=out_shape,
        scratch_shapes=scratch,
        compiler_params=pltpu.CompilerParams(dimension_semantics=("arbitrary",) * len(grid), vmem_limit_bytes=VMEM, **extra),
        cost_estimate=pl.CostEstimate(flops=int(flops), transcendentals=0, bytes_accessed=int(moved)),
    )(*args)


ROWS = lambda i: (i, 0)
COLS = lambda i: (0, i)
ONCE2 = lambda i: (0, 0)
ONCE4 = lambda i: (0, 0, 0, 0)


def _qkv_block(a, w, cos, sin, q_ref, k_ref, v_ref):
    d = a.shape[1]
    p = _dot(a, w(0, d)).astype(LOW).astype(WIDE)
    for n in range(d // HEAD):
        at = slice(n * HEAD, (n + 1) * HEAD)
        q_ref[:, at] = _turn(p[:, at], cos, sin)
    p = _dot(a, w(d, d + 2 * HEAD)).astype(LOW)
    k_ref[...] = _turn(p[:, :HEAD].astype(WIDE), cos, sin)
    v_ref[...] = p[:, HEAD:]


def _attend_block(iq, bq, q_s, k_s, v_s, o_ref, ot_ref, lse_ref, top_s, mix_s, halfway):
    d = o_ref.shape[1]
    heads, bk = d // HEAD, bq
    e = HEAD**-0.5 * LOG2E
    top_s[...] = jnp.full_like(top_s, NEG)
    mix_s[...] = jnp.zeros_like(mix_s)
    ones = jnp.ones((8, bk), LOW)
    mine = pl.ds(pl.multiple_of(iq * bq, bq), bq)

    def block(j, masked):
        here = pl.ds(pl.multiple_of(j * bk, bk), bk)
        scores = [_dot(k_s[here, :], q_s[mine, n * HEAD : (n + 1) * HEAD], 1, 1) for n in range(heads)]
        if masked:
            ok = lax.broadcasted_iota(jnp.int32, (bk, bq), 1) >= lax.broadcasted_iota(jnp.int32, (bk, bq), 0)
        weights, keeps = [], []
        for n, s in enumerate(scores):
            at = slice(n * bq, (n + 1) * bq)
            if masked:
                s = jnp.where(ok, s, HIDDEN)
            old = top_s[:, at]
            top = jnp.maximum(old, s.max(axis=0, keepdims=True))
            top_s[:, at] = top
            weights.append(jnp.exp2((s - top) * e).astype(LOW))
            keeps.append(jnp.exp2((old - top) * e))
        values = jnp.concatenate([v_s[here, :].T, ones], axis=0)
        for n, (p, keep) in enumerate(zip(weights, keeps)):
            at = slice(n * bq, (n + 1) * bq)
            mix_s[:, at] = mix_s[:, at] * keep + _dot(values, p)

    lax.fori_loop(0, iq, lambda j, _: block(j, False), None)
    halfway()
    block(iq, True)
    for n in range(heads):
        at = slice(n * bq, (n + 1) * bq)
        total = mix_s[HEAD : HEAD + 1, at]
        out = (mix_s[:HEAD, at] * (1 / total)).astype(LOW)
        ot_ref[n * HEAD : (n + 1) * HEAD, :] = out
        o_ref[:, n * HEAD : (n + 1) * HEAD] = out.T
        lse_ref[n : n + 1, :] = top_s[:, at] * HEAD**-0.5 + jnp.log(total)


def _keep(here, q_ref, k_ref, v_ref, q_s, k_s, v_s):
    q_s[here, :], k_s[here, :], v_s[here, :] = q_ref[...], k_ref[...], v_ref[...]


def _run(g, at, plan):
    for part in plan.split(";"):
        step, todo = part.split(":")
        pl.when(at == int(step))(lambda todo=todo: _stages(g, todo))


def _stages(g, todo):
    for at in range(0, len(todo), 2):
        g.stage(int(todo[at]), int(todo[at + 1]))


def _front_first_body(g, h_ref, freq_ref, q_ref, k_ref, v_ref, at_ref, cos_ref, sin_ref, o_ref, ot_ref, lse_ref,
                      w_s, a_s, cos_s, sin_s, q_s, k_s, v_s, top_s, mix_s, sem):
    bm = q_ref.shape[0]
    t = h_ref.shape[0]
    blocks = t // bm
    i = pl.program_id(0)

    @pl.when(i == 0)
    def _():
        g.greet()
        _stages(g, "00102001")

        def prepare(j, _):
            here = pl.ds(pl.multiple_of(j * bm, bm), bm)
            a_s[here, :] = _norm(h_ref[here, :])
            place = (lax.broadcasted_iota(jnp.int32, (bm, HEAD), 0) + j * bm).astype(WIDE)
            angle = place * freq_ref[...]
            cos_s[here, :] = jnp.cos(angle)
            sin = jnp.sin(angle)
            sin_s[here, :] = jnp.where(lax.broadcasted_iota(jnp.int32, (bm, HEAD), 1) < HEAD // 2, -sin, sin)

        lax.fori_loop(0, blocks, prepare, None)
        _stages(g, "020304051106121307140815")
        fetch = pltpu.make_async_copy(g.outs[0], w_s, sem)
        fetch.start()
        fetch.wait()

    _run(g, i, "1:21;2:2223;4:162425;6:17;7:26")

    @pl.when((i > 0) & (i <= blocks))
    def _():
        here = pl.ds(pl.multiple_of((i - 1) * bm, bm), bm)
        a = a_s[here, :]
        at_ref[...] = a.T
        cos, sin = cos_s[here, :], sin_s[here, :]
        cos_ref[...], sin_ref[...] = cos, sin
        _qkv_block(a, lambda x, y: w_s[:, :, :, x:y].reshape(a.shape[1], y - x), cos, sin, q_ref, k_ref, v_ref)
        _keep(here, q_ref, k_ref, v_ref, q_s, k_s, v_s)

    @pl.when(i > blocks)
    def _():
        _attend_block(i - blocks - 1, bm, q_s, k_s, v_s, o_ref, ot_ref, lse_ref, top_s, mix_s, lambda: _run(g, i, "8:1827"))

    _run(g, i, "8:28")


def _kept(t, d):
    return [pltpu.VMEM((t, d), LOW), pltpu.VMEM((t, HEAD), LOW), pltpu.VMEM((t, HEAD), LOW)]


def _front_outs(t, d, bm, late):
    blocks = t // bm
    first = lambda i: jnp.clip(i - late + blocks, 0, blocks - 1)
    second = lambda i: jnp.clip(i - late, 0, blocks - 1)
    rows = lambda at, n, dtype: ((t, n), dtype, (bm, n), lambda i: (at(i), 0))
    cols = lambda at, n, dtype: ((n, t), dtype, (n, bm), lambda i: (0, at(i)))
    return ([rows(first, d, LOW), rows(first, HEAD, LOW), rows(first, HEAD, LOW), cols(first, d, LOW)],
            [rows(second, d, LOW), cols(second, d, LOW), cols(second, d // HEAD, WIDE)], rows(first, HEAD, WIDE), rows(first, d, LOW), first)


def front_first(h, freq, gather, bm=512):
    t, d = h.shape
    early, late, table, _, _ = _front_outs(t, d, bm, t // bm + 1)
    return _call(
        _front_first_body, (2 * (t // bm) + 1,), [(h, (t, d), ONCE2), (freq, freq.shape, ONCE2)], early + [table, table] + late,
        [pltpu.VMEM((4, 2, d // 8, 2 * (d + HEAD)), LOW), pltpu.VMEM((t, d), LOW), pltpu.VMEM((t, HEAD), WIDE), pltpu.VMEM((t, HEAD), WIDE), *_kept(t, d),
         pltpu.VMEM((1, d // HEAD * bm), WIDE), pltpu.VMEM((HEAD + 8, d // HEAD * bm), WIDE), pltpu.SemaphoreType.DMA],
        flops=2 * t * d * (d + 2 * HEAD) * 5 + 4 * t * t * d, gather=gather)


def _front_body(g, h1_ref, act_ref, wd_ref, wa_ref, cos_ref, sin_ref, h_ref, q_ref, k_ref, v_ref, at_ref, o_ref, ot_ref, lse_ref,
                q_s, k_s, v_s, top_s, mix_s):
    bm = q_ref.shape[0]
    blocks = q_s.shape[0] // bm
    i = pl.program_id(0)

    @pl.when(i == 0)
    def _():
        g.greet()
        _stages(g, "00011011")

    _run(g, i, "2:02030405;3:12;4:0613;5:1415;6:07;7:0816")

    @pl.when(i < blocks)
    def _():
        h = _add(h1_ref[...], _dot(act_ref[...], wd_ref[...]).astype(LOW))
        h_ref[...] = h
        a = _norm(h)
        at_ref[...] = a.T
        _qkv_block(a, lambda x, y: wa_ref[:, x:y], cos_ref[...], sin_ref[...], q_ref, k_ref, v_ref)
        _keep(pl.ds(pl.multiple_of(i * bm, bm), bm), q_ref, k_ref, v_ref, q_s, k_s, v_s)

    @pl.when(i >= blocks)
    def _():
        _attend_block(i - blocks, bm, q_s, k_s, v_s, o_ref, ot_ref, lse_ref, top_s, mix_s, lambda: _run(g, i, "7:17"))

    _run(g, i, "7:18")


def front(h1, act, wd, wa, cos, sin, gather, bm=512):
    t, d = h1.shape
    early, late, _, rows, at = _front_outs(t, d, bm, t // bm)
    block = lambda a: (a, (bm, a.shape[1]), lambda i: (at(i), 0))
    return _call(
        _front_body, (2 * (t // bm),),
        [block(h1), block(act), (wd, wd.shape, ONCE2), (wa, wa.shape, ONCE2), block(cos), block(sin)], [rows] + early + late,
        [*_kept(t, d), pltpu.VMEM((1, d // HEAD * bm), WIDE), pltpu.VMEM((HEAD + 8, d // HEAD * bm), WIDE)],
        flops=2 * t * d * (d + 2 * HEAD + act.shape[1]) + 4 * t * t * d, gather=gather)


def _attend_bwd_body(q_ref, k_ref, v_ref, do_ref, lse_ref, delta_ref, cos_ref, sin_ref, dq_ref, dkv_ref, dq_s, dk_s, dv_s):
    bq, d = q_ref.shape
    heads, bk = d // HEAD, bq
    iq = pl.program_id(0)
    scale = HEAD**-0.5
    e = scale * LOG2E
    low = lambda x: x.astype(LOW)
    back = lambda x, here: _turn(low(x).astype(WIDE), cos_ref[here, :], -sin_ref[here, :])

    @pl.when(iq == 0)
    def _():
        dk_s[...] = jnp.zeros_like(dk_s)
        dv_s[...] = jnp.zeros_like(dv_s)

    dq_s[...] = jnp.zeros_like(dq_s)
    part = lambda ref, n: ref[:, n * HEAD : (n + 1) * HEAD]

    def block(j, masked):
        here = pl.ds(pl.multiple_of(j * bk, bk), bk)
        qs, dos = [part(q_ref, n) for n in range(heads)], [part(do_ref, n) for n in range(heads)]
        keys, values = k_ref[here, :], v_ref[here, :]
        scores = [_dot(keys, x, 1, 1) for x in qs]
        dps = [_dot(values, x, 1, 1) for x in dos]
        if masked:
            ok = lax.broadcasted_iota(jnp.int32, (bk, bq), 1) >= lax.broadcasted_iota(jnp.int32, (bk, bq), 0)
        for n in range(heads):
            p = jnp.exp2(scores[n] * e - lse_ref[n : n + 1, :] * LOG2E)
            if masked:
                p = jnp.where(ok, p, 0.0)
            ds = low(p * (dps[n] - delta_ref[n : n + 1, :]))
            dv_s[here, :] += _dot(low(p), dos[n])
            dk_s[here, :] += _dot(ds, qs[n])
            dq_s[:, n * bq : (n + 1) * bq] += _dot(keys.T, ds)

    lax.fori_loop(0, iq, lambda j, _: block(j, False), None)
    block(iq, True)
    mine = pl.ds(pl.multiple_of(iq * bq, bq), bq)
    for n in range(heads):
        dq_ref[:, n * HEAD : (n + 1) * HEAD] = back((dq_s[:, n * bq : (n + 1) * bq] * scale).T, mine)

    @pl.when(iq == pl.num_programs(0) - 1)
    def _():
        dkv_ref[:, :HEAD] = back(dk_s[...] * scale, slice(None))
        dkv_ref[:, HEAD:] = low(dv_s[...])


def attend_bwd(q, k, v, do, lse, delta, cos, sin, bq=256):
    t, d = q.shape
    stats = (d // HEAD, bq)
    return _call(
        _attend_bwd_body, (t // bq,),
        [(q, (bq, d), ROWS), (k, k.shape, ONCE2), (v, v.shape, ONCE2), (do, (bq, d), ROWS), (lse, stats, COLS), (delta, stats, COLS),
         (cos, cos.shape, ONCE2), (sin, sin.shape, ONCE2)],
        [((t, d), LOW, (bq, d), ROWS), ((t, 2 * HEAD), LOW, (t, 2 * HEAD), ONCE2)],
        [pltpu.VMEM((HEAD, d // HEAD * bq), WIDE), pltpu.VMEM(k.shape, WIDE), pltpu.VMEM(v.shape, WIDE)],
        flops=2 * t * t * d * 5)


def _silu(gate):
    sig = 0.5 * jnp.tanh(0.5 * gate) + 0.5
    return sig, gate * sig


CHUNK = 512


def _hidden(h_ref, o_ref, wa_ref, h1_ref, bt_ref):
    d = h_ref.shape[1]
    h1 = _add(h_ref[...], _dot(o_ref[...], wa_ref[:, d + 2 * HEAD :]).astype(LOW))
    h1_ref[...] = h1
    b = _norm(h1)
    bt_ref[...] = b.T
    return b


def _mlp_body(g, h_ref, o_ref, wa_ref, wg_ref, wu_ref, h1_ref, bt_ref, by_gate_ref, by_up_ref, act_ref):
    i = pl.program_id(0)
    pl.when(i == 0)(g.greet)
    _run(g, i, "0:0001;2:02;4:030405;6:06;7:07")
    b = _hidden(h_ref, o_ref, wa_ref, h1_ref, bt_ref)
    for at in range(0, wg_ref.shape[1], CHUNK):
        at = slice(at, at + CHUNK)
        gate, up = _dot(b, wg_ref[:, at]), _dot(b, wu_ref[:, at])
        by_gate_ref[:, at], by_up_ref[:, at] = by_gate, s = _slopes(gate, up)
        act_ref[:, at] = (s * up).astype(LOW)
    _run(g, i, "7:08")


def mlp(h, o, wa, wg, wu, gather, bm=256):
    t, d = h.shape
    f = wg.shape[1]
    return _call(
        _mlp_body, (t // bm,),
        [(h, (bm, d), ROWS), (o, (bm, d), ROWS), (wa, wa.shape, ONCE2), (wg, wg.shape, ONCE2), (wu, wu.shape, ONCE2)],
        [((t, d), LOW, (bm, d), ROWS), ((d, t), LOW, (d, bm), COLS), ((t, f), WIDE, (bm, f), ROWS), ((t, f), WIDE, (bm, f), ROWS),
         ((t, f), LOW, (bm, f), ROWS)],
        flops=2 * t * d * (d + 2 * f), gather=gather)


def _slopes(gate, up):
    sig, s = _silu(gate)
    return up * (sig + s * (1 - sig)), s


def _gates(dact, by_gate, by_up, dg_ref, du_ref, at):
    dact = dact.astype(LOW).astype(WIDE)
    dg_ref[:, at] = (dact * by_gate).astype(LOW)
    du_ref[:, at] = (dact * by_up).astype(LOW)


def _mlp_last_body(h_ref, o_ref, dy_ref, wa_ref, wg_ref, wu_ref, wd_ref, h1_ref, bt_ref, dyt_ref, act_ref, dg_ref, du_ref):
    dy = dy_ref[...]
    dyt_ref[...] = dy.T
    b = _hidden(h_ref, o_ref, wa_ref, h1_ref, bt_ref)
    for at in range(0, wg_ref.shape[1], CHUNK):
        at = slice(at, at + CHUNK)
        gate, up = _dot(b, wg_ref[:, at]), _dot(b, wu_ref[:, at])
        by_gate, s = _slopes(gate, up)
        _gates(_dot(dy, wd_ref[at, :], 1, 1), by_gate, s, dg_ref, du_ref, at)
        act_ref[:, at] = (s * up).astype(LOW)


def mlp_last(h, o, dy, wa, wg, wu, wd, bm=256):
    t, d = h.shape
    f = wg.shape[1]
    row, col, wide = ((t, d), LOW, (bm, d), ROWS), ((d, t), LOW, (d, bm), COLS), ((t, f), LOW, (bm, f), ROWS)
    return _call(
        _mlp_last_body, (t // bm,),
        [(h, (bm, d), ROWS), (o, (bm, d), ROWS), (dy, (bm, d), ROWS), (wa, wa.shape, ONCE2), (wg, wg.shape, ONCE2), (wu, wu.shape, ONCE2),
         (wd, wd.shape, ONCE2)],
        [row, col, col, wide, wide, wide], flops=2 * t * d * (d + 3 * f))


def _gates_bwd_body(dy_ref, by_gate_ref, by_up_ref, wd_ref, dg_ref, du_ref):
    dy = dy_ref[...]
    for at in range(0, by_gate_ref.shape[1], CHUNK):
        at = slice(at, at + CHUNK)
        _gates(_dot(dy, wd_ref[at, :], 1, 1), by_gate_ref[:, at], by_up_ref[:, at], dg_ref, du_ref, at)


def gates_bwd(dy, gate, up, wd, bm=256):
    t, d = dy.shape
    f = gate.shape[1]
    return _call(
        _gates_bwd_body, (t // bm,),
        [(dy, (bm, d), ROWS), (gate, (bm, f), ROWS), (up, (bm, f), ROWS), (wd, wd.shape, ONCE2)],
        [((t, f), LOW, (bm, f), ROWS), ((t, f), LOW, (bm, f), ROWS)],
        flops=2 * t * d * f)


def _mlp_bwd_body(dg_ref, du_ref, h1_ref, o_ref, dy_ref, wa_ref, wg_ref, wu_ref, dh1_ref, do_ref, delta_ref):
    half = dg_ref.shape[0] // 2
    d = dh1_ref.shape[1]
    halves = [slice(0, half), slice(half, None)]
    by = lambda r, w_ref, g_ref: _dot(w_ref[...], g_ref[r, :], 1, 1).astype(LOW)
    dbs = [_add(by(r, wg_ref, dg_ref), by(r, wu_ref, du_ref)).T for r in halves]
    for r, db in zip(halves, dbs):
        dh1 = _add(dy_ref[r, :], _norm_bwd(h1_ref[r, :], db))
        dh1_ref[r, :] = dh1
        do = _dot(dh1, wa_ref[:, d + 2 * HEAD :], 1, 1).astype(LOW)
        do_ref[r, :] = do
        both = do.astype(WIDE) * o_ref[r, :].astype(WIDE)
        for n in range(d // HEAD):
            delta_ref[n : n + 1, r] = jnp.sum(both[:, n * HEAD : (n + 1) * HEAD].T, 0, keepdims=True)


def mlp_bwd(dg, du, h1, o, dy, wa, wg, wu, bm=512):
    t, d = h1.shape
    f = wg.shape[1]
    return _call(
        _mlp_bwd_body, (t // bm,),
        [(dg, (bm, f), ROWS), (du, (bm, f), ROWS), (h1, (bm, d), ROWS), (o, (bm, d), ROWS), (dy, (bm, d), ROWS), (wa, wa.shape, ONCE2),
         (wg, wg.shape, ONCE2), (wu, wu.shape, ONCE2)],
        [((t, d), LOW, (bm, d), ROWS), ((t, d), LOW, (bm, d), ROWS), ((d // HEAD, t), WIDE, (d // HEAD, bm), COLS)],
        flops=2 * t * d * (d + 2 * f))


def _qkv_bwd_body(dq_ref, dkv_ref, h_ref, dh1_ref, w_ref, dh_ref, *dht_ref):
    d = dq_ref.shape[1]
    by = lambda g, a: _dot(w_ref[:, a : a + g.shape[1]], g, 1, 1).astype(LOW)
    da = _add(by(dkv_ref[:, HEAD:], d + HEAD), _add(by(dkv_ref[:, :HEAD], d), by(dq_ref[...], 0))).T
    dh = _add(dh1_ref[...], _norm_bwd(h_ref[...], da))
    dh_ref[...] = dh
    if dht_ref:
        dht_ref[0][...] = dh.T


def qkv_bwd(dq, dkv, h, dh1, wa, turned, bm=512):
    t, d = h.shape
    return _call(
        _qkv_bwd_body, (t // bm,),
        [(dq, (bm, d), ROWS), (dkv, (bm, 2 * HEAD), ROWS), (h, (bm, d), ROWS), (dh1, (bm, d), ROWS), (wa, wa.shape, ONCE2)],
        [((t, d), LOW, (bm, d), ROWS)] + ([((d, t), LOW, (d, bm), COLS)] if turned else []),
        flops=2 * t * d * (d + 2 * HEAD))


class Swap:
    def __init__(self, tile_s, out_s, in_s, send, recv, free):
        self.tile_s, self.out_s, self.in_s, self.send, self.recv, self.free = tile_s, out_s, in_s, send, recv, free
        dp = lax.axis_index("dp")
        self.core = dp % 2
        self.to = (lax.axis_index("rep"), dp + 1 - 2 * (dp % 2))

    @staticmethod
    def scratch(shape):
        z, rows, cols = shape
        return [pltpu.VMEM((2, z, 2, rows, cols), WIDE), pltpu.VMEM((2, *shape), LOW), pltpu.VMEM((2, *shape), LOW), pltpu.SemaphoreType.DMA((2,)),
                pltpu.SemaphoreType.DMA((2,)), pltpu.SemaphoreType.REGULAR]

    def copy(self, slot):
        return pltpu.make_async_remote_copy(src_ref=self.out_s.at[slot], dst_ref=self.in_s.at[slot], send_sem=self.send.at[slot],
                                            recv_sem=self.recv.at[slot], device_id=self.to, device_id_type=MESH)

    def step(self, n, tile, out_ref):
        i = pl.program_id(0)
        slot = i % 2

        @pl.when(i == 0)
        def _():
            barrier = pltpu.get_barrier_semaphore()
            pl.semaphore_signal(barrier, inc=1, device_id=self.to, device_id_type=MESH)
            pl.semaphore_wait(barrier, 1)

        @pl.when(i < n)
        def _():
            tile(i, self.tile_s.at[slot])
            pl.when(i >= 2)(lambda: self.copy(slot).wait_send())
            self.out_s[slot] = self.tile_s[slot, :, 1 - self.core].astype(LOW)

        @pl.when(i > 0)
        def _():
            self.copy(1 - slot).wait_recv()
            out_ref[...] = (self.tile_s[1 - slot, :, self.core] + self.in_s[1 - slot].astype(WIDE)).astype(LOW)
            pl.when(i + 1 < n)(lambda: pl.semaphore_signal(self.free, inc=1, device_id=self.to, device_id_type=MESH))

        @pl.when(i < n)
        def _():
            pl.when(i >= 2)(lambda: pl.semaphore_wait(self.free, 1))
            self.copy(slot).start()

        @pl.when(i == n)
        def _():
            for last in range(min(n, 2)):
                self.copy(last).wait_send()


def _grad_body(at_ref, *refs, plan):
    n = len({b for step in plan for b, _, _ in step})
    b_refs, out_ref = refs[:n], refs[n]
    swap = Swap(*refs[n + 1 :])

    def tile(i, ref):
        z, cores, rows, t = at_ref.shape
        a = at_ref[...].reshape(z * cores * rows, t)
        same = {}
        for at, step in enumerate(plan):
            same.setdefault(step, []).append(at)
        for step, ats in same.items():
            @pl.when((i >= ats[0]) & (i <= ats[-1]))
            def _(step=step):
                at = 0
                for b, first, width in step:
                    ref[:, :, :, at : at + width] = _dot(a, b_refs[b][:, first : first + width]).reshape(z, cores, rows, width)
                    at += width

    swap.step(len(plan), tile, out_ref)


def grad(at, bs, plan, cid):
    m, t = at.shape
    bn = sum(w for _, _, w in plan[0])
    specs = [(b, (t, w), lambda i, lo=lo, hi=b.shape[1] // w - 1: (0, jnp.clip(i - lo, 0, hi))) for b, w, lo in bs]
    tile = (4, m // 8, bn)
    n = len(plan)
    return _call(functools.partial(_grad_body, plan=plan), (n + 1,), [(at.reshape(4, 2, m // 8, t), (4, 2, m // 8, t), ONCE4)] + specs,
                 [((4, m // 8, n * bn), LOW, tile, lambda i: (0, 0, jnp.maximum(i - 1, 0)))], Swap.scratch(tile), flops=2 * t * m * n * bn,
                 collective_id=cid)[0]


def _grad_flip_body(at_ref, b_ref, out_ref, *refs):
    def tile(i, ref):
        ref[...] = _dot(at_ref[...], b_ref[...]).T.reshape(ref.shape)

    Swap(*refs).step(4, tile, out_ref)


def grad_flip(at, b, cid):
    m, t = at.shape
    n = b.shape[1]
    tile = (1, n // 8, m)
    return _call(_grad_flip_body, (5,), [(at, at.shape, ONCE2), (b, (t, n // 4), lambda i: (0, jnp.minimum(i, 3)))],
                 [((4, n // 8, m), LOW, tile, lambda i: (jnp.maximum(i - 1, 0), 0, 0))], Swap.scratch(tile), flops=2 * t * m * n,
                 collective_id=cid)[0]


def scatter(*parts):
    g = parts[0] if len(parts) == 1 else jnp.concatenate(parts, 2)
    return lax.psum_scatter(g.reshape(-1, g.shape[2]), "dp", scatter_dimension=0, tiled=True, axis_index_groups=[[0, 2, 4, 6], [1, 3, 5, 7]])


def solution(mesh):
    def layers(x, dy, wq, wk, wv, wo, w_gate, w_up, w_down):
        h, dh = x[0], dy[0]
        _, d = h.shape
        freq = THETA ** (-jnp.arange(HEAD // 2, dtype=WIDE) / (HEAD // 2))
        freq = jnp.concatenate([freq, freq])[None]
        w_all = jnp.concatenate([wq, wk, wv, wo], 2)
        whole = lambda w: lax.all_gather(w, "dp", axis=0, tiled=True)
        flat = lambda w: w.reshape(-1, w.shape[-1])

        def everywhere(w):
            rows = w.shape[0] // REPS
            return lax.all_gather(lax.dynamic_slice_in_dim(w, lax.axis_index("rep") * rows, rows), ("dp", "rep"), axis=0, tiled=True)

        both = lambda *xs: lax.optimization_barrier(xs)

        q, k, v, at, cos, sin, o, ot, lse, wa0, wg0, wu0 = front_first(h, freq, (0, [("cols", w_all, 0), ("cols", w_gate, 0), ("cols", w_up, 0)]))
        wa0, wg0, wu0 = flat(wa0), flat(wg0), flat(wu0)
        wa1 = whole(w_all[1])
        wd1 = everywhere(w_down[1])
        h1, bt, gate, up, act, wd0 = mlp(h, o, wa0, wg0, wu0, (1, [("rows", w_down, 0)]))
        wd0 = flat(wd0)
        kept = [(h, q, k, v, at, o, ot, lse, h1, bt, wa0, wg0, wu0)]
        h, q, k, v, at, o, ot, lse, wg1, wu1 = front(h1, act, wd0, wa1, cos, sin, (2, [("cols", w_gate, 1), ("cols", w_up, 1)]))
        wg1, wu1 = flat(wg1), flat(wu1)
        h1, bt, dht, act1, dg, du = mlp_last(h, o, dh, wa1, wg1, wu1, wd1)
        kept.append((h, q, k, v, at, o, ot, lse, h1, bt, wa1, wg1, wu1))

        mine = [None, None]
        f = act.shape[1]
        tiles = tuple(((b, 0, CHUNK),) for b in range(2) for _ in range(f // CHUNK))
        third = 3 * HEAD
        turned = (((0, 0, third),), ((0, 0, third),), ((1, 0, HEAD), (2, 0, 2 * HEAD)))
        for n in (1, 0):
            h, q, k, v, at, o, ot, lse, h1, bt, wa, wg, wu = kept[n]
            cid = 4 + 4 * n
            g_down = grad_flip(dht, (act, act1)[n], cid)
            if n:
                g_down, dg, du = both(g_down, dg, du)
            else:
                g_down, dh = both(g_down, dh)
            g_down = scatter(g_down)
            if not n:
                dg, du = gates_bwd(dh, gate, up, wd0)
            g_gate_up = grad(bt, [(dg, CHUNK, 0), (du, CHUNK, f // CHUNK)], tiles, cid + 1)
            g_gate_up, dg, du = both(g_gate_up, dg, du)
            g_gate_up = scatter(g_gate_up)
            dh1, do, delta = mlp_bwd(dg, du, h1, o, dh, wa, wg, wu)
            g_o, do = both(grad(ot, [(dh1, d, 0)], (((0, 0, d),),), cid + 2), do)
            if not n:
                g_o = scatter(g_o)
            dq, dkv = attend_bwd(q, k, v, do, lse, delta, cos, sin)
            g_qkv = grad(at, [(dq, third, 0), (dq[:, 2 * third :], HEAD, 0), (dkv, 2 * HEAD, 0)], turned, cid + 3)
            g_qkv, dkv = both(g_qkv, dkv)
            g_all = scatter(g_qkv, g_o) if n else scatter(g_qkv)
            dh, *dht = qkv_bwd(dq, dkv, h, dh1, wa, n > 0)
            if n:
                g_o, dht = g_all[:, d + 2 * HEAD :], dht[0]
            mine[n] = (g_all[:, :d], g_all[:, d : d + HEAD], g_all[:, d + HEAD : d + 2 * HEAD], g_o, g_gate_up[:, :f], g_gate_up[:, f:], g_down)
        return (dh[None], *(jnp.stack([mine[n][i] for n in range(2)]) for i in range(7)))

    states, cut = P(("rep", "dp"), None, None), P(None, "dp", None)
    return jax.shard_map(
        layers,
        mesh=mesh,
        in_specs=(states, states) + (cut,) * 7,
        out_specs=(states,) + (P("rep", "dp", None),) * 7,
        check_vma=False,
    )
```

```python
import functools

import jax
import jax.numpy as jnp
from jax import lax
from jax.experimental import pallas as pl
from jax.experimental.pallas import tpu as pltpu
from jax.sharding import PartitionSpec as P


HEAD = 128
THETA = 10000
LOG2E = 1.4426950408889634
NEG = -1e30
HIDDEN = 2 * NEG
VMEM = 60 * 2**20
MESH = pl.DeviceIdType.MESH
REPS = 4
LOW, WIDE = jnp.bfloat16, jnp.float32


def _dot(a, b, ca=1, cb=0):
    return lax.dot_general(a, b, (((ca,), (cb,)), ((), ())), preferred_element_type=WIDE)


def _scale(x):
    return lax.rsqrt(jnp.mean(x * x, -1, keepdims=True) + 1e-6)


def _norm(h):
    x = h.astype(WIDE)
    return (x * _scale(x)).astype(LOW)


def _norm_bwd(h, d):
    x, d = h.astype(WIDE), d.astype(WIDE)
    s = _scale(x)
    along = jnp.sum(d * x, -1, keepdims=True) * (s * s * s * (1 / x.shape[-1]))
    return (d * s - x * along).astype(LOW)


def _add(a, b):
    return (a.astype(WIDE) + b.astype(WIDE)).astype(LOW)


def _turn(t, cos, sin):
    return (t * cos + pltpu.roll(t, HEAD // 2, 1) * sin).astype(LOW)


class Gather:
    ORDER = "abcdefghijklmnopqrs"
    WHOLE = ("*+abc", "+dh", "-a+ei", "-b+fj", "-c+gk.+p", "-de+lm", "-jk+no-fg+q-hi+r", "-lmno+s", "-pqrs!")
    PLANS = {"": WHOLE, "side": ("*+abc", "-abc.!"), "quarter": ("+dhp*", "-d+lq-h+nr", "-ln+s", "-pqrs.!")}

    def __init__(self, pieces, outs, kinds, send, recv, local):
        self.pieces, self.outs, self.kinds, self.send, self.recv, self.local = pieces, outs, kinds, send, recv, local
        self.r, dp = lax.axis_index("rep"), lax.axis_index("dp")
        self.z, self.c = dp // 2, dp % 2
        self.rx, self.ry, self.rd = (self.r + 2) % 4, self.r + 1 - 2 * (self.r % 2), 3 - self.r
        self.here, self.partner = dp, (self.r, dp + 1 - 2 * self.c)

    def greet(self):
        barrier = pltpu.get_barrier_semaphore()
        others = [(self.r, (self.z + k) % 4 * 2 + self.c) for k in (1, 2, 3)]
        others += [(self.rx, self.here), (self.ry, self.here), self.partner]
        for rep, dp in others:
            pl.semaphore_signal(barrier, inc=1, device_id=(rep, dp), device_id_type=MESH)
        pl.semaphore_wait(barrier, len(others))

    def place(self, m, z, r):
        ref, kind, z = self.outs[m], self.kinds[m], pl.ds(0, 4) if z is None else z
        if "side" in kind:
            return ref.at[z]
        if "rows" in kind:
            return ref.at[z, self.c, r]
        width = self.pieces[m].shape[-1]
        return ref.at[z, self.c, :, pl.ds(pl.multiple_of(r * width, 128), width)]

    def copy(self, m, t):
        quarter = "quarter" in self.kinds[m]
        xs, ys = (self.rx, self.here), (self.ry, self.here)
        behind = lambda j: (self.z + 4 - j) % 4
        if t in "abc":
            of, to = (self.z, self.r), (self.r, (self.z + 1 + "abc".index(t)) % 4 * 2 + self.c)
        elif t in "pqrs":
            of, to = (None, (self.r, self.rx, self.ry, self.rd)["pqrs".index(t)]), self.partner
        elif t in "lm":
            of, to = (pl.ds(0, 2) if quarter else behind("lm".index(t)), self.rx), ys
        elif t in "no":
            of, to = (pl.ds(2, 2) if quarter else behind("..no".index(t)), self.ry), xs
        else:
            of, to = (None if quarter else behind(max("defg".find(t), "hijk".find(t))), self.r), xs if t in "defg" else ys
        dst = self.place(m, *of)
        src = self.pieces[m] if t in "abcdh" + "p" * quarter else dst
        at = self.ORDER.index(t)
        return pltpu.make_async_remote_copy(src_ref=src, dst_ref=dst, send_sem=self.send.at[m, at], recv_sem=self.recv.at[m, at],
                                            device_id=to, device_id_type=MESH)

    def stage(self, m, s):
        plan = self.PLANS[self.kinds[m][4:]]
        own = lambda: pltpu.make_async_copy(self.pieces[m], self.place(m, None if "quarter" in self.kinds[m] else self.z, self.r), self.local.at[m])
        for step in plan[s]:
            if step in "+-":
                mode = step
            elif step == "*":
                own().start()
            elif step == ".":
                own().wait()
            elif step == "!":
                for t in self.ORDER:
                    if any(t in x for x in plan):
                        self.copy(m, t).wait_send()
            elif mode == "+":
                self.copy(m, step).start()
            else:
                self.copy(m, step).wait_recv()


def _call(body, grid, ins, outs, scratch=(), flops=0, gather=None, collective_id=None):
    def spec(shape, block, at):
        whole = tuple(block) == tuple(shape)
        return pl.BlockSpec(block, at, pipeline_mode=pl.Buffered(1)) if whole else pl.BlockSpec(block, at)

    size = lambda s, t: functools.reduce(lambda x, y: x * y, s, 1) * jnp.dtype(t).itemsize
    moved = sum(size(a.shape, a.dtype) for a, _, _ in ins) + sum(size(s, t) for s, t, _, _ in outs)
    in_specs, args = [spec(a.shape, block, at) for a, block, at in ins], [a for a, _, _ in ins]
    out_specs = [pl.BlockSpec(block, at) for _, _, block, at in outs]
    out_shape = [jax.ShapeDtypeStruct(s, t) for s, t, _, _ in outs]
    scratch = list(scratch)
    extra = {} if collective_id is None else dict(collective_id=collective_id, has_side_effects=True)
    if gather is not None:
        cid, pieces = gather
        extra = dict(collective_id=cid, has_side_effects=True)
        for kind, array, n in pieces:
            rows, cols = array.shape[1:]
            cut = "rows" in kind
            if "quarter" in kind:
                block, at = array.shape, ONCE3
            elif cut:
                block, at = (1, rows // REPS, cols), lambda *i, n=n: (n, lax.axis_index("rep"), 0)
            else:
                block, at = (1, rows, cols // REPS), lambda *i, n=n: (n, 0, lax.axis_index("rep"))
            shape = (4, 2, REPS, *block[1:]) if cut else (4, 2, rows, REPS * block[2])
            if "side" in kind:
                shape = (4, *block[1:])
            in_specs.append(pl.BlockSpec(block, at, pipeline_mode=pl.Buffered(1)))
            args.append(array)
            out_specs.append(pl.BlockSpec(memory_space=pl.ANY))
            out_shape.append(jax.ShapeDtypeStruct(shape, array.dtype))
        m = len(pieces)
        count = (m, len(Gather.ORDER))
        scratch += [pltpu.SemaphoreType.DMA(count), pltpu.SemaphoreType.DMA(count), pltpu.SemaphoreType.DMA((m,))]
        inner, n_in, n_out = body, len(ins), len(outs)

        def body(*refs):
            mine, refs = refs[:n_in], refs[n_in:]
            parts, refs = refs[:m], refs[m:]
            results, refs = refs[:n_out], refs[n_out:]
            whole, refs = refs[:m], refs[m:]
            kinds = [k for k, _, _ in pieces]
            inner(Gather([p if "quarter" in k else p.at[0] for p, k in zip(parts, kinds)], whole, kinds, *refs[-3:]), *mine, *results, *refs[:-3])

    return pl.pallas_call(
        body,
        grid=grid,
        in_specs=in_specs,
        out_specs=out_specs,
        out_shape=out_shape,
        scratch_shapes=scratch,
        compiler_params=pltpu.CompilerParams(dimension_semantics=("arbitrary",) * len(grid), vmem_limit_bytes=VMEM, **extra),
        cost_estimate=pl.CostEstimate(flops=int(flops), transcendentals=0, bytes_accessed=int(moved)),
    )(*args)


ROWS = lambda i: (i, 0)
COLS = lambda i: (0, i)
ONCE2 = lambda i: (0, 0)
ONCE3 = lambda *i: (0, 0, 0)
ONCE4 = lambda i: (0, 0, 0, 0)


def _qkv_block(a, w, cos, sin, q_ref, k_ref, v_ref):
    d = a.shape[1]
    p = _dot(a, w(0, d)).astype(LOW).astype(WIDE)
    for n in range(d // HEAD):
        at = slice(n * HEAD, (n + 1) * HEAD)
        q_ref[:, at] = _turn(p[:, at], cos, sin)
    p = _dot(a, w(d, d + 2 * HEAD)).astype(LOW)
    k_ref[...] = _turn(p[:, :HEAD].astype(WIDE), cos, sin)
    v_ref[...] = p[:, HEAD:]


def _attend_block(iq, bq, q_s, k_s, v_s, o_ref, ot_ref, lse_ref, top_s, mix_s, halfway):
    d = o_ref.shape[1]
    heads = d // HEAD
    e = HEAD**-0.5 * LOG2E
    top_s[...] = jnp.full_like(top_s, NEG)
    mix_s[...] = jnp.zeros_like(mix_s)
    half = bq // 2

    def block(first, bk, lo, diagonal):
        here = pl.ds(pl.multiple_of(first, bk), bk)
        mine = pl.ds(pl.multiple_of(iq * bq + lo, half), bq - lo)
        scores = [_dot(k_s[here, :], q_s[mine, n * HEAD : (n + 1) * HEAD], 1, 1) for n in range(heads)]
        if diagonal is not None:
            ok = lax.broadcasted_iota(jnp.int32, scores[0].shape, 1) + (lo - diagonal) >= lax.broadcasted_iota(jnp.int32, scores[0].shape, 0)
        weights, keeps = [], []
        for n, s in enumerate(scores):
            at = slice(n * bq + lo, (n + 1) * bq)
            if diagonal is not None:
                s = jnp.where(ok, s, HIDDEN)
            old = top_s[:, at]
            top = jnp.maximum(old, s.max(axis=0, keepdims=True))
            top_s[:, at] = top
            weights.append(jnp.exp2((s - top) * e).astype(LOW))
            keeps.append(jnp.exp2((old - top) * e))
        values = jnp.concatenate([v_s[here, :].T, jnp.ones((8, bk), LOW)], axis=0)
        for n, (p, keep) in enumerate(zip(weights, keeps)):
            at = slice(n * bq + lo, (n + 1) * bq)
            mix_s[:, at] = mix_s[:, at] * keep + _dot(values, p)

    lax.fori_loop(0, iq, lambda j, _: block(j * bq, bq, 0, None), None)
    halfway()
    block(iq * bq, half, 0, 0)
    block(iq * bq + half, half, half, half)
    for n in range(heads):
        at = slice(n * bq, (n + 1) * bq)
        total = mix_s[HEAD : HEAD + 1, at]
        out = (mix_s[:HEAD, at] * (1 / total)).astype(LOW)
        ot_ref[n * HEAD : (n + 1) * HEAD, :] = out
        o_ref[:, n * HEAD : (n + 1) * HEAD] = out.T
        lse_ref[n : n + 1, :] = top_s[:, at] * HEAD**-0.5 + jnp.log(total)


def _keep(here, q_ref, k_ref, v_ref, q_s, k_s, v_s):
    q_s[here, :], k_s[here, :], v_s[here, :] = q_ref[...], k_ref[...], v_ref[...]


def _run(g, at, plan):
    for part in plan.split(";"):
        step, todo = part.split(":")
        pl.when(at == int(step))(lambda todo=todo: _stages(g, todo))


def _stages(g, todo):
    for at in range(0, len(todo), 2):
        g.stage(int(todo[at]), int(todo[at + 1]))


def _front_first_body(g, h_ref, freq_ref, q_ref, k_ref, v_ref, at_ref, cos_ref, sin_ref, o_ref, ot_ref, lse_ref,
                      w_s, a_s, cos_s, sin_s, q_s, k_s, v_s, top_s, mix_s, sem):
    bm = q_ref.shape[0]
    t = h_ref.shape[0]
    blocks = t // bm
    i = pl.program_id(0)

    @pl.when(i == 0)
    def _():
        g.greet()
        _stages(g, "00102001")

        def normed(j, _):
            here = pl.ds(pl.multiple_of(j * bm, bm), bm)
            a_s[here, :] = _norm(h_ref[here, :])

        def tables(j, _):
            here = pl.ds(pl.multiple_of(j * bm, bm), bm)
            place = (lax.broadcasted_iota(jnp.int32, (bm, HEAD), 0) + j * bm).astype(WIDE)
            angle = place * freq_ref[...]
            cos_s[here, :] = jnp.cos(angle)
            sin = jnp.sin(angle)
            sin_s[here, :] = jnp.where(lax.broadcasted_iota(jnp.int32, (bm, HEAD), 1) < HEAD // 2, -sin, sin)

        lax.fori_loop(0, blocks, normed, None)
        _stages(g, "0203")
        lax.fori_loop(0, blocks // 2, tables, None)
        _stages(g, "040511")
        lax.fori_loop(blocks // 2, blocks, tables, None)
        _stages(g, "06121307140815")
        fetch = pltpu.make_async_copy(g.outs[0], w_s, sem)
        fetch.start()
        fetch.wait()

    _run(g, i, "1:21304050;2:2223;4:162425;6:17;7:26")

    @pl.when((i > 0) & (i <= blocks))
    def _():
        here = pl.ds(pl.multiple_of((i - 1) * bm, bm), bm)
        a = a_s[here, :]
        at_ref[...] = a.T
        cos, sin = cos_s[here, :], sin_s[here, :]
        cos_ref[...], sin_ref[...] = cos, sin
        _qkv_block(a, lambda x, y: w_s[:, :, :, x:y].reshape(a.shape[1], y - x), cos, sin, q_ref, k_ref, v_ref)
        _keep(here, q_ref, k_ref, v_ref, q_s, k_s, v_s)

    @pl.when(i > blocks)
    def _():
        _attend_block(i - blocks - 1, bm, q_s, k_s, v_s, o_ref, ot_ref, lse_ref, top_s, mix_s, lambda: _run(g, i, "8:1827"))

    _run(g, i, "8:28314151")


def _kept(t, d):
    return [pltpu.VMEM((t, d), LOW), pltpu.VMEM((t, HEAD), LOW), pltpu.VMEM((t, HEAD), LOW)]


def _front_outs(t, d, bm, late):
    blocks = t // bm
    first = lambda i: jnp.clip(i - late + blocks, 0, blocks - 1)
    second = lambda i: jnp.clip(i - late, 0, blocks - 1)
    rows = lambda at, n, dtype: ((t, n), dtype, (bm, n), lambda i: (at(i), 0))
    cols = lambda at, n, dtype: ((n, t), dtype, (n, bm), lambda i: (0, at(i)))
    return ([rows(first, d, LOW), rows(first, HEAD, LOW), rows(first, HEAD, LOW), cols(first, d, LOW)],
            [rows(second, d, LOW), cols(second, d, LOW), cols(second, d // HEAD, WIDE)], rows(first, HEAD, WIDE), rows(first, d, LOW), first)


def front_first(h, freq, gather, bm=512):
    t, d = h.shape
    early, late, table, _, _ = _front_outs(t, d, bm, t // bm + 1)
    return _call(
        _front_first_body, (2 * (t // bm) + 1,), [(h, (t, d), ONCE2), (freq, freq.shape, ONCE2)], early + [table, table] + late,
        [pltpu.VMEM((4, 2, d // 8, 2 * (d + HEAD)), LOW), pltpu.VMEM((t, d), LOW), pltpu.VMEM((t, HEAD), WIDE), pltpu.VMEM((t, HEAD), WIDE), *_kept(t, d),
         pltpu.VMEM((1, d // HEAD * bm), WIDE), pltpu.VMEM((HEAD + 8, d // HEAD * bm), WIDE), pltpu.SemaphoreType.DMA],
        flops=2 * t * d * (d + 2 * HEAD) * 5 + 4 * t * t * d, gather=gather)


def _front_body(g, h1_ref, act_ref, wd_ref, wa_ref, cos_ref, sin_ref, h_ref, q_ref, k_ref, v_ref, at_ref, o_ref, ot_ref, lse_ref,
                q_s, k_s, v_s, top_s, mix_s):
    bm = q_ref.shape[0]
    blocks = q_s.shape[0] // bm
    i = pl.program_id(0)

    @pl.when(i == 0)
    def _():
        g.greet()
        _stages(g, "0010")

    _run(g, i, "4:01;6:11;7:02")

    @pl.when(i < blocks)
    def _():
        h = _add(h1_ref[...], _dot(act_ref[...], wd_ref[...]).astype(LOW))
        h_ref[...] = h
        a = _norm(h)
        at_ref[...] = a.T
        _qkv_block(a, lambda x, y: wa_ref[:, x:y], cos_ref[...], sin_ref[...], q_ref, k_ref, v_ref)
        _keep(pl.ds(pl.multiple_of(i * bm, bm), bm), q_ref, k_ref, v_ref, q_s, k_s, v_s)

    @pl.when(i >= blocks)
    def _():
        _attend_block(i - blocks, bm, q_s, k_s, v_s, o_ref, ot_ref, lse_ref, top_s, mix_s, lambda: _run(g, i, "7:12"))

    _run(g, i, "7:1303")


def front(h1, act, wd, wa, cos, sin, gather, bm=512):
    t, d = h1.shape
    early, late, _, rows, at = _front_outs(t, d, bm, t // bm)
    block = lambda a: (a, (bm, a.shape[1]), lambda i: (at(i), 0))
    return _call(
        _front_body, (2 * (t // bm),),
        [block(h1), block(act), (wd, wd.shape, ONCE2), (wa, wa.shape, ONCE2), block(cos), block(sin)], [rows] + early + late,
        [*_kept(t, d), pltpu.VMEM((1, d // HEAD * bm), WIDE), pltpu.VMEM((HEAD + 8, d // HEAD * bm), WIDE)],
        flops=2 * t * d * (d + 2 * HEAD + act.shape[1]) + 4 * t * t * d, gather=gather)


def _attend_bwd_body(q_ref, k_ref, v_ref, do_ref, lse_ref, delta_ref, cos_ref, sin_ref, dq_ref, dkv_ref, lse_s, delta_s, dq_s, dk_s, dv_s):
    bq, d = q_ref.shape
    heads = d // HEAD
    iq = pl.program_id(0)
    scale = HEAD**-0.5
    low = lambda x: x.astype(LOW)
    back = lambda x, here: _turn(low(x).astype(WIDE), cos_ref[here, :], -sin_ref[here, :])
    part = lambda n: slice(n * HEAD, (n + 1) * HEAD)
    rows = lambda n: slice(n * bq, (n + 1) * bq)
    below = lambda x: jnp.concatenate([x[:, part(n)] for n in range(heads)], 0)
    aside = lambda x: jnp.concatenate([x[part(n), :] for n in range(heads)], 1)

    @pl.when(iq == 0)
    def _():
        dk_s[...] = jnp.zeros_like(dk_s)
        dv_s[...] = jnp.zeros_like(dv_s)

    dq_s[...] = jnp.zeros_like(dq_s)
    for n in range(heads):
        spread = lambda ref: jnp.broadcast_to(ref[n : n + 1, :], (HEAD, bq)).T
        lse_s[rows(n), :] = spread(lse_ref) * LOG2E
        delta_s[rows(n), :] = spread(delta_ref)

    def block(first, bk, lo, diagonal):
        here = pl.ds(pl.multiple_of(first, bk), bk)
        q, do = q_ref[lo:, :], do_ref[lo:, :]
        nq = bq - lo
        keys, values = k_ref[here, :], v_ref[here, :]
        scores, dps = _dot(below(q), keys, 1, 1), _dot(below(do), values, 1, 1)
        if diagonal is not None:
            ok = lax.broadcasted_iota(jnp.int32, (nq, bk), 0) + (lo - diagonal) >= lax.broadcasted_iota(jnp.int32, (nq, bk), 1)
        ps, dss = [], []
        for n in range(heads):
            mine = slice(n * nq, (n + 1) * nq)
            wide = lambda ref: jnp.concatenate([ref[n * bq + lo : (n + 1) * bq, :]] * (bk // HEAD), 1)
            p = jnp.exp2(scores[mine] * (scale * LOG2E) - wide(lse_s))
            if diagonal is not None:
                p = jnp.where(ok, p, 0.0)
            ps.append(low(p))
            dss.append(low(p * (dps[mine] - wide(delta_s))))
        p, ds = jnp.concatenate(ps, 0), jnp.concatenate(dss, 0)
        dv_s[:, here] += _dot(aside(do.T), p)
        dk_s[:, here] += _dot(aside(q.T), ds)
        by_q = _dot(ds, keys)
        for n in range(heads):
            dq_s[n * bq + lo : (n + 1) * bq, :] += by_q[n * nq : (n + 1) * nq]

    half = bq // 2
    lax.fori_loop(0, iq, lambda j, _: block(j * bq, bq, 0, None), None)
    block(iq * bq, half, 0, 0)
    block(iq * bq + half, half, half, half)
    mine = pl.ds(pl.multiple_of(iq * bq, bq), bq)
    for n in range(heads):
        dq_ref[:, part(n)] = back(dq_s[rows(n), :] * scale, mine)

    @pl.when(iq == pl.num_programs(0) - 1)
    def _():
        dkv_ref[:, :HEAD] = back((dk_s[...] * scale).T, slice(None))
        dkv_ref[:, HEAD:] = low(dv_s[...].T)


def attend_bwd(q, k, v, do, lse, delta, cos, sin, bq=512):
    t, d = q.shape
    stats = (d // HEAD, bq)
    column = pltpu.VMEM((d // HEAD * bq, HEAD), WIDE)
    return _call(
        _attend_bwd_body, (t // bq,),
        [(q, (bq, d), ROWS), (k, k.shape, ONCE2), (v, v.shape, ONCE2), (do, (bq, d), ROWS), (lse, stats, COLS), (delta, stats, COLS),
         (cos, cos.shape, ONCE2), (sin, sin.shape, ONCE2)],
        [((t, d), LOW, (bq, d), ROWS), ((t, 2 * HEAD), LOW, (t, 2 * HEAD), ONCE2)],
        [column, column, column, pltpu.VMEM((HEAD, t), WIDE), pltpu.VMEM((HEAD, t), WIDE)],
        flops=2 * t * t * d * 5)


def _pack_body(*refs):
    *ws, first_ref, second_ref = refs
    for n, out in enumerate((first_ref, second_ref)):
        at = 0
        for ref in ws:
            out[0, :, at : at + ref.shape[2]] = ref[n]
            at += ref.shape[2]


def pack(*ws):
    rows, n = ws[0].shape[1], sum(w.shape[2] for w in ws)
    return _call(_pack_body, (1,), [(w, w.shape, ONCE3) for w in ws],
                 [((1, rows, n), LOW, (1, rows, n), ONCE3)] * 2)


def _silu(gate):
    sig = 0.5 * jnp.tanh(0.5 * gate) + 0.5
    return sig, gate * sig


CHUNK = 512


def _hidden(h_ref, o_ref, wa_ref, h1_ref, bt_ref):
    d = h_ref.shape[1]
    h1 = _add(h_ref[...], _dot(o_ref[...], wa_ref[:, -d:]).astype(LOW))
    h1_ref[...] = h1
    b = _norm(h1)
    bt_ref[...] = b.T
    return b


def _mlp_body(g, h_ref, o_ref, wa_ref, wg_ref, wu_ref, h1_ref, bt_ref, by_gate_ref, by_up_ref, act_ref):
    i = pl.program_id(0)
    pl.when(i == 0)(g.greet)
    _run(g, i, "0:00;4:01;6:02")
    b = _hidden(h_ref, o_ref, wa_ref, h1_ref, bt_ref)
    for at in range(0, wg_ref.shape[1], CHUNK):
        at = slice(at, at + CHUNK)
        gate, up = _dot(b, wg_ref[:, at]), _dot(b, wu_ref[:, at])
        by_gate_ref[:, at], by_up_ref[:, at] = by_gate, s = _slopes(gate, up)
        act_ref[:, at] = (s * up).astype(LOW)
    _run(g, i, "7:03")


def mlp(h, o, wa, wg, wu, gather, bm=256):
    t, d = h.shape
    f = wg.shape[1]
    return _call(
        _mlp_body, (t // bm,),
        [(h, (bm, d), ROWS), (o, (bm, d), ROWS), (wa, (d, wa.shape[1] // 2), lambda i: (0, 1)), (wg, wg.shape, ONCE2), (wu, wu.shape, ONCE2)],
        [((t, d), LOW, (bm, d), ROWS), ((d, t), LOW, (d, bm), COLS), ((t, f), WIDE, (bm, f), ROWS), ((t, f), WIDE, (bm, f), ROWS),
         ((t, f), LOW, (bm, f), ROWS)],
        flops=2 * t * d * (d + 2 * f), gather=gather)


def _slopes(gate, up):
    sig, s = _silu(gate)
    return up * (sig + s * (1 - sig)), s


def _gates(dact, by_gate, by_up, dg_ref, du_ref, at):
    dact = dact.astype(LOW).astype(WIDE)
    dg_ref[:, at] = (dact * by_gate).astype(LOW)
    du_ref[:, at] = (dact * by_up).astype(LOW)


def _mlp_last_body(h_ref, o_ref, dy_ref, wa_ref, wg_ref, wu_ref, wd_ref, h1_ref, bt_ref, dyt_ref, act_ref, dg_ref, du_ref):
    dy = dy_ref[...]
    dyt_ref[...] = dy.T
    b = _hidden(h_ref, o_ref, wa_ref, h1_ref, bt_ref)
    for at in range(0, wg_ref.shape[1], CHUNK):
        at = slice(at, at + CHUNK)
        gate, up = _dot(b, wg_ref[:, at]), _dot(b, wu_ref[:, at])
        by_gate, s = _slopes(gate, up)
        _gates(_dot(dy, wd_ref[at, :], 1, 1), by_gate, s, dg_ref, du_ref, at)
        act_ref[:, at] = (s * up).astype(LOW)


def mlp_last(h, o, dy, wa, wg, wu, wd, bm=256):
    t, d = h.shape
    f = wg.shape[1]
    row, col, wide = ((t, d), LOW, (bm, d), ROWS), ((d, t), LOW, (d, bm), COLS), ((t, f), LOW, (bm, f), ROWS)
    return _call(
        _mlp_last_body, (t // bm,),
        [(h, (bm, d), ROWS), (o, (bm, d), ROWS), (dy, (bm, d), ROWS), (wa, (d, wa.shape[1] // 2), lambda i: (0, 1)), (wg, wg.shape, ONCE2), (wu, wu.shape, ONCE2),
         (wd, wd.shape, ONCE2)],
        [row, col, col, wide, wide, wide], flops=2 * t * d * (d + 3 * f))


def _gates_bwd_body(dy_ref, by_gate_ref, by_up_ref, wd_ref, dg_ref, du_ref):
    dy = dy_ref[...]
    for at in range(0, by_gate_ref.shape[1], CHUNK):
        at = slice(at, at + CHUNK)
        _gates(_dot(dy, wd_ref[at, :], 1, 1), by_gate_ref[:, at], by_up_ref[:, at], dg_ref, du_ref, at)


def gates_bwd(dy, gate, up, wd, bm=256):
    t, d = dy.shape
    f = gate.shape[1]
    return _call(
        _gates_bwd_body, (t // bm,),
        [(dy, (bm, d), ROWS), (gate, (bm, f), ROWS), (up, (bm, f), ROWS), (wd, wd.shape, ONCE2)],
        [((t, f), LOW, (bm, f), ROWS), ((t, f), LOW, (bm, f), ROWS)],
        flops=2 * t * d * f)


def _mlp_bwd_body(dg_ref, du_ref, h1_ref, o_ref, dy_ref, wa_ref, wg_ref, wu_ref, dh1_ref, do_ref, delta_ref):
    half = dg_ref.shape[0] // 2
    d = dh1_ref.shape[1]
    halves = [slice(0, half), slice(half, None)]
    by = lambda r, w_ref, g_ref: _dot(w_ref[...], g_ref[r, :], 1, 1).astype(LOW)
    dbs = [_add(by(r, wg_ref, dg_ref), by(r, wu_ref, du_ref)).T for r in halves]
    for r, db in zip(halves, dbs):
        dh1 = _add(dy_ref[r, :], _norm_bwd(h1_ref[r, :], db))
        dh1_ref[r, :] = dh1
        do = _dot(dh1, wa_ref[:, -d:], 1, 1).astype(LOW)
        do_ref[r, :] = do
        both = do.astype(WIDE) * o_ref[r, :].astype(WIDE)
        for n in range(d // HEAD):
            delta_ref[n : n + 1, r] = jnp.sum(both[:, n * HEAD : (n + 1) * HEAD].T, 0, keepdims=True)


def mlp_bwd(dg, du, h1, o, dy, wa, wg, wu, bm=512):
    t, d = h1.shape
    f = wg.shape[1]
    return _call(
        _mlp_bwd_body, (t // bm,),
        [(dg, (bm, f), ROWS), (du, (bm, f), ROWS), (h1, (bm, d), ROWS), (o, (bm, d), ROWS), (dy, (bm, d), ROWS), (wa, (d, wa.shape[1] // 2), lambda i: (0, 1)),
         (wg, wg.shape, ONCE2), (wu, wu.shape, ONCE2)],
        [((t, d), LOW, (bm, d), ROWS), ((t, d), LOW, (bm, d), ROWS), ((d // HEAD, t), WIDE, (d // HEAD, bm), COLS)],
        flops=2 * t * d * (d + 2 * f))


def _qkv_bwd_body(dq_ref, dkv_ref, h_ref, dh1_ref, w_ref, dh_ref, *dht_ref):
    d = dq_ref.shape[1]
    by = lambda g, a: _dot(w_ref[:, a : a + g.shape[1]], g, 1, 1).astype(LOW)
    da = _add(by(dkv_ref[:, HEAD:], d + HEAD), _add(by(dkv_ref[:, :HEAD], d), by(dq_ref[...], 0))).T
    dh = _add(dh1_ref[...], _norm_bwd(h_ref[...], da))
    dh_ref[...] = dh
    if dht_ref:
        dht_ref[0][...] = dh.T


def qkv_bwd(dq, dkv, h, dh1, wa, turned, bm=512):
    t, d = h.shape
    return _call(
        _qkv_bwd_body, (t // bm,),
        [(dq, (bm, d), ROWS), (dkv, (bm, 2 * HEAD), ROWS), (h, (bm, d), ROWS), (dh1, (bm, d), ROWS), (wa, wa.shape, ONCE2)],
        [((t, d), LOW, (bm, d), ROWS)] + ([((d, t), LOW, (d, bm), COLS)] if turned else []),
        flops=2 * t * d * (d + 2 * HEAD))


class Swap:
    def __init__(self, tile_s, out_s, in_s, send, recv, free):
        self.tile_s, self.out_s, self.in_s, self.send, self.recv, self.free = tile_s, out_s, in_s, send, recv, free
        dp = lax.axis_index("dp")
        self.core = dp % 2
        self.to = (lax.axis_index("rep"), dp + 1 - 2 * (dp % 2))

    @staticmethod
    def scratch(shape):
        z, rows, cols = shape
        return [pltpu.VMEM((2, z, 2, rows, cols), WIDE), pltpu.VMEM((2, *shape), LOW), pltpu.VMEM((2, *shape), LOW), pltpu.SemaphoreType.DMA((2,)),
                pltpu.SemaphoreType.DMA((2,)), pltpu.SemaphoreType.REGULAR]

    def copy(self, slot):
        return pltpu.make_async_remote_copy(src_ref=self.out_s.at[slot], dst_ref=self.in_s.at[slot], send_sem=self.send.at[slot],
                                            recv_sem=self.recv.at[slot], device_id=self.to, device_id_type=MESH)

    def step(self, n, tile, out_ref):
        i = pl.program_id(0)
        slot = i % 2

        @pl.when(i == 0)
        def _():
            barrier = pltpu.get_barrier_semaphore()
            pl.semaphore_signal(barrier, inc=1, device_id=self.to, device_id_type=MESH)
            pl.semaphore_wait(barrier, 1)

        @pl.when(i < n)
        def _():
            tile(i, self.tile_s.at[slot])
            pl.when(i >= 2)(lambda: self.copy(slot).wait_send())
            self.out_s[slot] = self.tile_s[slot, :, 1 - self.core].astype(LOW)

        @pl.when(i > 0)
        def _():
            self.copy(1 - slot).wait_recv()
            out_ref[...] = (self.tile_s[1 - slot, :, self.core] + self.in_s[1 - slot].astype(WIDE)).astype(LOW)
            pl.when(i + 1 < n)(lambda: pl.semaphore_signal(self.free, inc=1, device_id=self.to, device_id_type=MESH))

        @pl.when(i < n)
        def _():
            pl.when(i >= 2)(lambda: pl.semaphore_wait(self.free, 1))
            self.copy(slot).start()

        @pl.when(i == n)
        def _():
            for last in range(min(n, 2)):
                self.copy(last).wait_send()


def _grad_body(at_ref, *refs, plan):
    n = len({b for step in plan for b, _, _ in step})
    b_refs, out_ref = refs[:n], refs[n]
    swap = Swap(*refs[n + 1 :])

    def tile(i, ref):
        z, cores, rows, t = at_ref.shape
        a = at_ref[...].reshape(z * cores * rows, t)
        same = {}
        for at, step in enumerate(plan):
            same.setdefault(step, []).append(at)
        for step, ats in same.items():
            @pl.when((i >= ats[0]) & (i <= ats[-1]))
            def _(step=step):
                at = 0
                for b, first, width in step:
                    ref[:, :, :, at : at + width] = _dot(a, b_refs[b][:, first : first + width]).reshape(z, cores, rows, width)
                    at += width

    swap.step(len(plan), tile, out_ref)


def grad(at, bs, plan, cid):
    m, t = at.shape
    bn = sum(w for _, _, w in plan[0])
    specs = [(b, (t, w), lambda i, lo=lo, hi=b.shape[1] // w - 1: (0, jnp.clip(i - lo, 0, hi))) for b, w, lo in bs]
    tile = (4, m // 8, bn)
    n = len(plan)
    return _call(functools.partial(_grad_body, plan=plan), (n + 1,), [(at.reshape(4, 2, m // 8, t), (4, 2, m // 8, t), ONCE4)] + specs,
                 [((4, m // 8, n * bn), LOW, tile, lambda i: (0, 0, jnp.maximum(i - 1, 0)))], Swap.scratch(tile), flops=2 * t * m * n * bn,
                 collective_id=cid)[0]


def _grad_flip_body(at_ref, b_ref, out_ref, *refs):
    def tile(i, ref):
        ref[...] = _dot(at_ref[...], b_ref[...]).T.reshape(ref.shape)

    Swap(*refs).step(4, tile, out_ref)


def grad_flip(at, b, cid):
    m, t = at.shape
    n = b.shape[1]
    tile = (1, n // 8, m)
    return _call(_grad_flip_body, (5,), [(at, at.shape, ONCE2), (b, (t, n // 4), lambda i: (0, jnp.minimum(i, 3)))],
                 [((4, n // 8, m), LOW, tile, lambda i: (jnp.maximum(i - 1, 0), 0, 0))], Swap.scratch(tile), flops=2 * t * m * n,
                 collective_id=cid)[0]


def scatter(*parts):
    g = parts[0] if len(parts) == 1 else jnp.concatenate(parts, 2)
    return lax.psum_scatter(g.reshape(-1, g.shape[2]), "dp", scatter_dimension=0, tiled=True, axis_index_groups=[[0, 2, 4, 6], [1, 3, 5, 7]])


def solution(mesh):
    def layers(x, dy, wq, wk, wv, wo, w_gate, w_up, w_down):
        h, dh = x[0], dy[0]
        _, d = h.shape
        freq = THETA ** (-jnp.arange(HEAD // 2, dtype=WIDE) / (HEAD // 2))
        freq = jnp.concatenate([freq, freq])[None]
        w_first, w_second = pack(wq, wk, wv, wo)
        whole = lambda w: lax.all_gather(w, "dp", axis=0, tiled=True)
        flat = lambda w: w.reshape(-1, w.shape[-1])

        both = lambda *xs: lax.optimization_barrier(xs)

        q, k, v, at, cos, sin, o, ot, lse, wa0, wg0, wu0, *sides = front_first(h, freq, (0, [
            ("cols", w_first, 0), ("cols", w_gate, 0), ("cols", w_up, 0), ("colsside", w_gate, 1), ("colsside", w_up, 1),
            ("rowsside", w_down, 0)]))
        wa0, wg0, wu0 = flat(wa0), flat(wg0), flat(wu0)
        wa1 = whole(w_second[0])
        wd1 = whole(w_down[1])
        h1, bt, gate, up, act, wd0 = mlp(h, o, wa0, wg0, wu0, (1, [("rowsquarter", sides[2], 0)]))
        wd0 = flat(wd0)
        kept = [(h, q, k, v, at, o, ot, lse, h1, bt, wa0, wg0, wu0)]
        h, q, k, v, at, o, ot, lse, wg1, wu1 = front(h1, act, wd0, wa1, cos, sin, (2, [("colsquarter", sides[0], 0), ("colsquarter", sides[1], 0)]))
        wg1, wu1 = flat(wg1), flat(wu1)
        h1, bt, dht, act1, dg, du = mlp_last(h, o, dh, wa1, wg1, wu1, wd1)
        kept.append((h, q, k, v, at, o, ot, lse, h1, bt, wa1, wg1, wu1))

        mine = [None, None]
        f = act.shape[1]
        tiles = tuple(((b, 0, CHUNK),) for b in range(2) for _ in range(f // CHUNK))
        third = 3 * HEAD
        turned = (((0, 0, third),), ((0, 0, third),), ((1, 0, HEAD), (2, 0, 2 * HEAD)))
        for n in (1, 0):
            h, q, k, v, at, o, ot, lse, h1, bt, wa, wg, wu = kept[n]
            cid = 4 + 4 * n
            g_down = grad_flip(dht, (act, act1)[n], cid)
            if n:
                g_down, dg, du = both(g_down, dg, du)
            else:
                g_down, dh = both(g_down, dh)
            g_down = scatter(g_down)
            if not n:
                dg, du = gates_bwd(dh, gate, up, wd0)
            g_gate_up = grad(bt, [(dg, CHUNK, 0), (du, CHUNK, f // CHUNK)], tiles, cid + 1)
            g_gate_up, dg, du = both(g_gate_up, dg, du)
            g_gate_up = scatter(g_gate_up)
            dh1, do, delta = mlp_bwd(dg, du, h1, o, dh, wa, wg, wu)
            g_o, do = both(grad(ot, [(dh1, d, 0)], (((0, 0, d),),), cid + 2), do)
            if not n:
                g_o = scatter(g_o)
            dq, dkv = attend_bwd(q, k, v, do, lse, delta, cos, sin)
            g_qkv = grad(at, [(dq, third, 0), (dq, HEAD, 1 - d // HEAD), (dkv, 2 * HEAD, 0)], turned, cid + 3)
            g_qkv, dkv = both(g_qkv, dkv)
            g_all = scatter(g_qkv, g_o) if n else scatter(g_qkv)
            dh, *dht = qkv_bwd(dq, dkv, h, dh1, wa, n > 0)
            if n:
                g_o, dht = g_all[:, d + 2 * HEAD :], dht[0]
            mine[n] = (g_all[:, :d], g_all[:, d : d + HEAD], g_all[:, d + HEAD : d + 2 * HEAD], g_o, g_gate_up[:, :f], g_gate_up[:, f:], g_down)
        return (dh[None], *(jnp.stack([mine[n][i] for n in range(2)]) for i in range(7)))

    states, cut = P(("rep", "dp"), None, None), P(None, "dp", None)
    return jax.shard_map(
        layers,
        mesh=mesh,
        in_specs=(states, states) + (cut,) * 7,
        out_specs=(states,) + (P("rep", "dp", None),) * 7,
        check_vma=False,
    )
```
